256 devices in a mesh: fsdp: 16 (over z, core), tp: 16 (over y, x).
Axes of the slice: x: 4, y: 4, z: 8, core: 2. Of those that a mesh axis runs over, the one named last changes fastest.
Arguments:
- w_gate: bfloat16 [4096, 11008], P('fsdp', 'tp'), may hold values from -0.09375 to 0.09375
- low_gate: bfloat16 [4096, 16], P('fsdp'), may hold values from -0.09375 to 0.09375
- high_gate: bfloat16 [16, 11008], P(None, 'tp'), may hold values from -1.5 to 1.5
- w_up: bfloat16 [4096, 11008], P('fsdp', 'tp'), may hold values from -0.09375 to 0.09375
- low_up: bfloat16 [4096, 16], P('fsdp'), may hold values from -0.09375 to 0.09375
- high_up: bfloat16 [16, 11008], P(None, 'tp'), may hold values from -1.5 to 1.5
- w_down: bfloat16 [11008, 4096], P('tp', 'fsdp'), may hold values from -0.0546875 to 0.0546875
- low_down: bfloat16 [11008, 16], P('tp'), may hold values from -0.0546875 to 0.0546875
- high_down: bfloat16 [16, 4096], P(None, 'fsdp'), may hold values from -1.5 to 1.5
- norm_train: float32 [4096], P(('fsdp', 'tp')), may hold values from 0.25 to 1.75
- norm_step: float32 [4096], P(('fsdp', 'tp')), may hold values from -0.3 to 0.3
Outputs:
- serving_gate: bfloat16 [4096, 11008], P(None, 'tp')
- serving_up: bfloat16 [4096, 11008], P(None, 'tp')
- serving_down: bfloat16 [11008, 4096], P('tp')
- serve_norm: bfloat16 [4096], replicated
The draws below stay inside these ranges and needn't reach their ends.
All inputs are finite; a program needn't handle non-finite values.
Results may differ from the reference program's by a relative error of at most 0.001.
Values may be sent and summed in bfloat16 or wider, within the bound.
A program may use at most 128 MiB of HBM per device.

```python
import jax
import jax.numpy as jnp

D_MODEL = 4096
D_INNER = 11008
RANK = 16


def shard_levels(rng, dims, pieces, low, high):
    level = 1.0
    for position, parts in pieces:
        steps = jax.random.uniform(jax.random.fold_in(jax.random.fold_in(rng, 6), position), (parts,), jnp.float32, low / len(pieces), high / len(pieces))
        level = level * jnp.repeat(jnp.exp(steps), dims[position] // parts).reshape((-1,) + (1,) * (len(dims) - 1 - position))
    return level


def gaussian(stream_key, shape, scale, limit, shards=(), kind=jnp.bfloat16):
    level = shard_levels(stream_key, shape, shards, -0.22, 0.18) if shards else 1.0
    entries = jax.random.normal(stream_key, shape, jnp.float32) * scale * level
    return jnp.minimum(jnp.maximum(entries, -limit), limit).astype(kind)


def setup_inputs(seed: int = 0) -> dict:
    seeds = jax.random.split(jax.random.key(seed), 12)
    return {
        "w_gate": gaussian(seeds[0], (D_MODEL, D_INNER), D_MODEL ** -0.5, 0.09375, ((0, 16), (1, 16))),
        "low_gate": gaussian(seeds[1], (D_MODEL, RANK), D_MODEL ** -0.5, 0.09375, ((0, 16),)),
        "high_gate": gaussian(seeds[2], (RANK, D_INNER), RANK ** -0.5, 1.5, ((1, 16),)),
        "w_up": gaussian(seeds[3], (D_MODEL, D_INNER), D_MODEL ** -0.5, 0.09375, ((0, 16), (1, 16))),
        "low_up": gaussian(seeds[4], (D_MODEL, RANK), D_MODEL ** -0.5, 0.09375, ((0, 16),)),
        "high_up": gaussian(seeds[5], (RANK, D_INNER), RANK ** -0.5, 1.5, ((1, 16),)),
        "w_down": gaussian(seeds[6], (D_INNER, D_MODEL), D_INNER ** -0.5, 0.0546875, ((0, 16), (1, 16))),
        "low_down": gaussian(seeds[7], (D_INNER, RANK), D_INNER ** -0.5, 0.0546875, ((0, 16),)),
        "high_down": gaussian(seeds[8], (RANK, D_MODEL), RANK ** -0.5, 1.5, ((1, 16),)),
        "norm_train": jnp.clip(1.0 + 0.15 * jax.random.normal(seeds[9], (D_MODEL,), jnp.float32), 0.25, 1.75),
        "norm_step": jnp.clip(jax.random.uniform(seeds[10], (D_MODEL,), jnp.float32, -0.3, 0.3) * shard_levels(seeds[10], (D_MODEL,), ((0, 256),), -0.4, 0.0), -0.3, 0.3),
    }


mix_rate = 2.0


def reference(w_gate, low_gate, high_gate, w_up, low_up, high_up, w_down, low_down, high_down, norm_train, norm_step):
    whole_gate = w_gate.astype(jnp.float32) + mix_rate * jnp.dot(low_gate, high_gate, preferred_element_type=jnp.float32)
    whole_up = w_up.astype(jnp.float32) + mix_rate * jnp.dot(low_up, high_up, preferred_element_type=jnp.float32)
    whole_down = w_down.astype(jnp.float32) + mix_rate * jnp.dot(low_down, high_down, preferred_element_type=jnp.float32)
    serving_gate = whole_gate.astype(jnp.bfloat16)
    serving_up = whole_up.astype(jnp.bfloat16)
    serving_down = whole_down.astype(jnp.bfloat16)
    serve_norm = (norm_train + norm_step).astype(jnp.bfloat16)
    return serving_gate, serving_up, serving_down, serve_norm
```

```python
import functools

import jax
import jax.numpy as jnp
from jax import lax
from jax.experimental import pallas as pl
from jax.experimental.pallas import tpu as pltpu
from jax.sharding import Mesh
from jax.sharding import PartitionSpec as P

mix_rate = 2.0
MESH = pl.DeviceIdType.MESH
AXES = ("z", "core", "y", "x")
FSDP = ("z", "core")
TP = ("y", "x")
NZ, NX, NY = 8, 4, 4
ROWS = ((0, 384), (384, 304))
TILE = 128


def body(rows_total, width, *refs):
    (wg, wu, wd, ag, au, ad, bg, bu, bd, ntrain, nstep, og, ou, od, onorm,
     w_v, a_v, b_v, own, nt_v, ns_v, nz, nsib, nx, ny, nrow,
     in_sem, own_sem, r_recv, l_recv, s_recv, own_send, r_send, l_send, s_send,
     nrr, nlr, nrs, nls, nsr, nss, nxr, nxs, nyr, nys) = refs
    w_hbm, a_hbm, b_hbm, outs = (wg, wu, wd), (ag, au, ad), (bg, bu, bd), (og, ou, od)
    z, core, y, x = (lax.axis_index(k) for k in AXES)
    right, left = {"z": lax.rem(z + 1, NZ)}, {"z": lax.rem(z + NZ - 1, NZ)}
    sib = {"core": 1 - core}
    x_up, x_down = {"x": lax.rem(x + 1, NX)}, {"x": lax.rem(x + NX - 1, NX)}
    y_up, y_down = {"y": lax.rem(y + 1, NY)}, {"y": lax.rem(y + NY - 1, NY)}
    chunks = [(m, r0, n) for m in range(3) for r0, n in ROWS]
    count = len(chunks)

    loads = []
    for m in range(3):
        loads.append([
            pltpu.make_async_copy(w_hbm[m], w_v.at[m], in_sem.at[m, 0]),
            pltpu.make_async_copy(a_hbm[m], a_v.at[m], in_sem.at[m, 1]),
            pltpu.make_async_copy(b_hbm[m], b_v.at[m], in_sem.at[m, 2]),
        ])
    norm_loads = [
        pltpu.make_async_copy(ntrain, nt_v, in_sem.at[3, 0]),
        pltpu.make_async_copy(nstep, ns_v, in_sem.at[3, 1]),
    ]
    for m in range(3):
        for copy in loads[m]:
            copy.start()
    for copy in norm_loads:
        copy.start()

    barrier = pltpu.get_barrier_semaphore()
    for device in (right, left, sib, x_up, x_down, y_up, y_down):
        pl.semaphore_signal(barrier, inc=1, device_id=device, device_id_type=MESH)

    def columns(block_z, block_core):
        at = (block_z * 2 + block_core) * width
        return pl.ds(pl.multiple_of(at, width), width)

    def spot(k, block_z, block_core):
        m, r0, n = chunks[k]
        return outs[m].at[pl.ds(r0, n), columns(block_z, block_core)]

    def mine(k):
        m, r0, n = chunks[k]
        return own.at[m, pl.ds(r0, n), :]

    def remote(src, dst, send, recv, device):
        return pltpu.make_async_remote_copy(
            src_ref=src, dst_ref=dst, send_sem=send, recv_sem=recv, device_id=device, device_id_type=MESH)

    half = count // 2

    def r_copy(step, k):
        block = lax.rem(z + NZ - step, NZ)
        src = mine(k) if step == 0 else spot(k, block, core)
        return remote(src, spot(k, block, core), r_send.at[step, k], r_recv.at[step, k], right)

    def l_copy(step, k):
        block = lax.rem(z + step, NZ)
        src = mine(k) if step == 0 else spot(k, block, core)
        return remote(src, spot(k, block, core), l_send.at[step, k], l_recv.at[step, k], left)

    def arrived(sem, step, k, block):
        return remote(spot(k, block, core), spot(k, block, core), r_send.at[0, 0], sem.at[step, k], right)

    def s_copy(dist, k):
        block = lax.rem(z + dist, NZ)
        src = mine(k) if dist == 0 else spot(k, block, core)
        return remote(src, spot(k, block, core), s_send.at[dist, k], s_recv.at[dist, k], sib)

    def s_arrived(dist, k):
        block = lax.rem(z + dist, NZ)
        return remote(spot(k, block, 1 - core), spot(k, block, 1 - core), s_send.at[dist, k], s_recv.at[dist, k], sib)

    def compute(k):
        m, r0, n = chunks[k]
        for at in range(r0, r0 + n, TILE):
            size = min(TILE, r0 + n - at)
            delta = lax.dot_general(
                a_v[m, :, at:at + size], b_v[m], (((0,), (0,)), ((), ())), preferred_element_type=jnp.float32)
            whole = w_v[m, at:at + size, :].astype(jnp.float32) + mix_rate * delta
            own[m, at:at + size, :] = whole.astype(jnp.bfloat16)

    started = []

    def go(copy):
        copy.start()
        started.append(copy)

    own_copies = []

    def send_own(k):
        go(r_copy(0, k))
        go(l_copy(0, k))
        go(s_copy(0, k))
        copy = pltpu.make_async_copy(mine(k), spot(k, z, core), own_sem.at[k])
        copy.start()
        own_copies.append(copy)

    for k in range(count):
        m = chunks[k][0]
        if k == 0 or chunks[k - 1][0] != m:
            for copy in loads[m]:
                copy.wait()
        compute(k)
        if k == 1:
            pl.semaphore_wait(barrier, 7)
        if k >= 1:
            send_own(k - 1)

    for copy in norm_loads:
        copy.wait()
    gain = (nt_v[...] + ns_v[...]).astype(jnp.bfloat16)
    t = y * NX + x
    lane = lax.broadcasted_iota(jnp.int32, (16, 128), 1)
    entry = lax.broadcasted_iota(jnp.int32, (16, 128), 0)
    place = jnp.where(lane == lax.rem(t, 8) * 16 + entry, 1.0, 0.0).astype(jnp.bfloat16)
    spread = jnp.dot(jnp.broadcast_to(gain, (16, 16)), place, preferred_element_type=jnp.float32)[:8]
    row = lax.broadcasted_iota(jnp.int32, (8, 128), 0)
    nz[z] = jnp.where(row == core * 2 + t // 8, spread, 0.0)
    send_own(count - 1)

    def norm_r(step):
        block = lax.rem(z + NZ - step, NZ)
        return remote(nz.at[block], nz.at[block], nrs.at[step], nrr.at[step], right)

    def norm_r_arrived(step):
        block = lax.rem(z + NZ - step - 1, NZ)
        return remote(nz.at[block], nz.at[block], nrs.at[step], nrr.at[step], right)

    def norm_l(step):
        block = lax.rem(z + step, NZ)
        return remote(nz.at[block], nz.at[block], nls.at[step], nlr.at[step], left)

    def norm_l_arrived(step):
        block = lax.rem(z + step + 1, NZ)
        return remote(nz.at[block], nz.at[block], nls.at[step], nlr.at[step], left)

    def norm_start():
        go(norm_r(0))
        go(norm_l(0))

    def norm_step(step):
        def act():
            norm_r_arrived(step).wait_recv()
            if step < 3:
                go(norm_r(step + 1))
                norm_l_arrived(step).wait_recv()
                if step < 2:
                    go(norm_l(step + 1))
        return act

    sib_norm = remote(nz, nsib, nss, nsr, sib)

    def x_copy(step):
        return remote(nx.at[step], nx.at[step + 1], nxs.at[step], nxr.at[step], x_up)

    def y_copy(step):
        return remote(ny.at[step], ny.at[step + 1], nys.at[step], nyr.at[step], y_up)

    def norm_sib():
        go(sib_norm)

    def norm_x0():
        sib_norm.wait_recv()
        nx[0] = nz[...] + nsib[...]

    def norm_x(step):
        def act():
            if step > 0:
                x_copy(step - 1).wait_recv()
            if step < 3:
                go(x_copy(step))
            else:
                ny[0] = nx[0] + nx[1] + nx[2] + nx[3]
        return act

    def norm_y(step):
        def act():
            if step > 0:
                y_copy(step - 1).wait_recv()
            if step < 3:
                go(y_copy(step))
            else:
                whole = ny[0] + ny[1] + ny[2] + ny[3]
                for k in range(NZ):
                    nrow[4 * k:4 * k + 4, :] = whole[k, 0:4, :]
                onorm[...] = nrow[...].astype(jnp.bfloat16)
        return act

    acts = [norm_start] + [norm_step(k) for k in range(4)] + [norm_sib, norm_x0]
    acts += [norm_x(k) for k in range(4)] + [norm_y(k) for k in range(4)]

    for step in range(4):
        for k in range(count):
            if step < 3 or k < half:
                block = lax.rem(z + NZ - step - 1, NZ)
                arrived(r_recv, step, k, block).wait_recv()
                if step < 2 or (step == 2 and k < half):
                    go(r_copy(step + 1, k))
                go(s_copy(NZ - step - 1, k))
            if step < 3 or k >= half:
                block = lax.rem(z + step + 1, NZ)
                arrived(l_recv, step, k, block).wait_recv()
                if step < 2 or (step == 2 and k >= half):
                    go(l_copy(step + 1, k))
                go(s_copy(step + 1, k))
            if acts:
                acts.pop(0)()
    while acts:
        acts.pop(0)()

    for copy in own_copies:
        copy.wait()
    for copy in started:
        copy.wait_send()
    for dist in range(NZ):
        for k in range(count):
            s_arrived(dist, k).wait_recv()


def gathered(*args):
    w, a, b, norms = args[0:3], args[3:6], args[6:9], args[9:11]
    rows, width = w[0].shape
    rank = a[0].shape[0]
    count = 3 * len(ROWS)
    whole = jax.ShapeDtypeStruct((rows, width * 16), jnp.bfloat16)
    anywhere = pl.BlockSpec(memory_space=pl.ANY)
    dma = pltpu.SemaphoreType.DMA
    f32 = jnp.float32
    return pl.pallas_call(
        functools.partial(body, rows, width),
        out_shape=(whole, whole, whole, jax.ShapeDtypeStruct((32, 128), jnp.bfloat16)),
        in_specs=[anywhere] * 11,
        out_specs=(anywhere, anywhere, anywhere, pl.BlockSpec(memory_space=pltpu.VMEM)),
        scratch_shapes=[
            pltpu.VMEM((3, rows, width), jnp.bfloat16),
            pltpu.VMEM((3, rank, rows), jnp.bfloat16),
            pltpu.VMEM((3, rank, width), jnp.bfloat16),
            pltpu.VMEM((3, rows, width), jnp.bfloat16),
            pltpu.VMEM((1, 16), f32),
            pltpu.VMEM((1, 16), f32),
            pltpu.VMEM((8, 8, 128), f32),
            pltpu.VMEM((8, 8, 128), f32),
            pltpu.VMEM((4, 8, 8, 128), f32),
            pltpu.VMEM((4, 8, 8, 128), f32),
            pltpu.VMEM((32, 128), f32),
            dma((4, 3)), dma((count,)),
            dma((4, count)), dma((4, count)), dma((8, count)),
            dma((1,)), dma((4, count)), dma((4, count)), dma((8, count)),
            dma((4,)), dma((4,)), dma((4,)), dma((4,)),
            dma, dma, dma((3,)), dma((3,)), dma((3,)), dma((3,)),
        ],
        compiler_params=pltpu.CompilerParams(collective_id=0, has_side_effects=True),
        name="merge_and_gather",
    )(*w, *a, *b, *norms)


def local(w_gate, low_gate, high_gate, w_up, low_up, high_up, w_down, low_down, high_down, norm_train, norm_step):
    gate, up, down, norm = gathered(
        w_gate.T, w_up.T, w_down, high_gate, high_up, low_down.T, low_gate.T, low_up.T, high_down,
        norm_train.reshape(1, 16), norm_step.reshape(1, 16))
    return gate.T, up.T, down, norm.reshape(-1)


def solution(mesh):
    finer = Mesh(mesh.devices.reshape(8, 2, 4, 4), AXES)
    in_specs = (
        P(FSDP, TP), P(FSDP, None), P(None, TP),
        P(FSDP, TP), P(FSDP, None), P(None, TP),
        P(TP, FSDP), P(TP, None), P(None, FSDP),
        P(FSDP + TP), P(FSDP + TP),
    )
    out_specs = (P(None, TP), P(None, TP), P(TP, None), P())
    return jax.shard_map(local, mesh=finer, in_specs=in_specs, out_specs=out_specs, check_vma=False)
```

```python
import functools

import jax
import jax.numpy as jnp
from jax import lax
from jax.experimental import pallas as pl
from jax.experimental.pallas import tpu as pltpu
from jax.sharding import Mesh
from jax.sharding import PartitionSpec as P

mix_rate = 2.0
SHIFT = 0
LEAD = 2
NORM_AT = 3
MESH = pl.DeviceIdType.MESH
AXES = ("z", "core", "y", "x")
FSDP = ("z", "core")
TP = ("y", "x")
NZ, NX, NY = 8, 4, 4
PIECES = (((0, 344), (344, 344), (688, 344), (1032, 344), (1376, 344), (1720, 344)),) * 4
MOST = max(len(p) for p in PIECES)


def body(rows, *refs):
    (wg, wu, wd, ag, au, ad, bg, bu, bd, ntrain, nstep, blocks, onorm,
     w_v, a_v, b_v, nt_v, ns_v, nz, ncore, nx, ny, nrow,
     in_sem, r_recv, l_recv, s_recv, r_send, l_send, s_send,
     nrr, nlr, nrs, nls, nsr, nss, nxr, nxs, nyr, nys,
     right_in, left_in, x_in, y_in, sib_in) = refs
    w_hbm, a_hbm, b_hbm = (wg, wu, wd), (ag, au, ad), (bg, bu, bd)
    z, core, y, x = (lax.axis_index(k) for k in AXES)
    right, left = {"z": lax.rem(z + 1, NZ)}, {"z": lax.rem(z + NZ - 1, NZ)}
    sib = {"core": 1 - core}

    barrier = pltpu.get_barrier_semaphore()

    def maybe(cond, act):
        @pl.when(cond)
        def _():
            act()

    def signal(sem, device):
        pl.semaphore_signal(sem, inc=1, device_id=device, device_id_type=MESH)

    def greet(at, last, up, down):
        @pl.when(at < last)
        def _():
            signal(barrier, up)

        @pl.when(at == 0)
        def _():
            signal(barrier, down)

    greet(z, NZ - 1, right, left)

    @pl.when(core == 1)
    def _():
        signal(barrier, sib)

    loads = []
    for m in range(3):
        loads.append([
            pltpu.make_async_copy(w_hbm[m], w_v.at[m], in_sem.at[m, 0]),
            pltpu.make_async_copy(a_hbm[m], a_v.at[m], in_sem.at[m, 1]),
            pltpu.make_async_copy(b_hbm[m], b_v.at[m], in_sem.at[m, 2]),
        ])
    norm_loads = [
        pltpu.make_async_copy(ntrain, nt_v, in_sem.at[3, 0]),
        pltpu.make_async_copy(nstep, ns_v, in_sem.at[3, 1]),
    ]
    for m in range(3):
        for copy in loads[m]:
            copy.start()
    for copy in norm_loads:
        copy.start()
    for k in range(1, NX):
        maybe(x + k < NX, lambda: signal(barrier, {"x": x + k}))
    for k in range(1, NY):
        maybe(y + k < NY, lambda: signal(barrier, {"y": y + k}))

    def greeted():
        def least(at, last):
            return jnp.where(at > 0, 1, 0) + jnp.where(at == last, 1, 0)

        greetings = least(z, NZ - 1) + x + y + (1 - core)
        maybe(greetings > 0, lambda: pl.semaphore_wait(barrier, greetings))

        @pl.when(z > 0)
        def _():
            signal(right_in, left)

        @pl.when(z == NZ - 1)
        def _():
            signal(left_in, right)

        @pl.when(core == 0)
        def _():
            signal(sib_in, sib)

        for k in range(1, NX):
            maybe(x - k >= 0, lambda: signal(x_in, {"x": x - k}))
        for k in range(1, NY):
            maybe(y - k >= 0, lambda: signal(y_in, {"y": y - k}))

    def spot(step, k, block_z, block_core):
        r0, n = PIECES[step][k]
        return blocks.at[block_z * 2 + block_core, pl.ds(r0, n), :]

    def remote(src, dst, send, recv, device):
        return pltpu.make_async_remote_copy(
            src_ref=src, dst_ref=dst, send_sem=send, recv_sem=recv, device_id=device, device_id_type=MESH)

    count = len(PIECES[3])

    def split(at):
        return count // 2 + jnp.where(at == NZ - 1, SHIFT, 0) - jnp.where(at == 0, SHIFT, 0)

    r_out, r_in = split(lax.rem(z + 1, NZ)), split(z)
    l_out, l_in = split(lax.rem(z + NZ - 1, NZ)), split(z)
    low, high = count // 2 - SHIFT, count // 2 + SHIFT

    def r_copy(step, k):
        at = spot(step, k, lax.rem(z + NZ - step, NZ), core)
        return remote(at, at, r_send.at[step, k], r_recv.at[step, k], right)

    def l_copy(step, k):
        at = spot(step, k, lax.rem(z + step, NZ), core)
        return remote(at, at, l_send.at[step, k], l_recv.at[step, k], left)

    def r_wait(step, k):
        at = spot(step, k, lax.rem(z + NZ - step - 1, NZ), core)
        remote(at, at, r_send.at[step, k], r_recv.at[step, k], right).wait_recv()

    def l_wait(step, k):
        at = spot(step, k, lax.rem(z + step + 1, NZ), core)
        remote(at, at, l_send.at[step, k], l_recv.at[step, k], left).wait_recv()

    def table(dist):
        return max(min(dist, NZ - dist) - 1, 0)

    def s_copy(dist, k):
        at = spot(table(dist), k, lax.rem(z + dist, NZ), core)
        return remote(at, at, s_send.at[dist, k], s_recv.at[dist, k], sib)

    def s_wait(dist, k):
        at = spot(table(dist), k, lax.rem(z + dist, NZ), 1 - core)
        remote(at, at, s_send.at[dist, k], s_recv.at[dist, k], sib).wait_recv()

    loaded = set()

    def compute(k):
        r0, n = PIECES[0][k]
        for m in range(3):
            at, end = max(r0, m * rows) - m * rows, min(r0 + n, (m + 1) * rows) - m * rows
            if at >= end:
                continue
            if m not in loaded:
                loaded.add(m)
                for copy in loads[m]:
                    copy.wait()
            delta = lax.dot_general(
                a_v[m, :, at:end], b_v[m], (((0,), (0,)), ((), ())), preferred_element_type=jnp.float32)
            whole = w_v[m, at:end, :].astype(jnp.float32) + mix_rate * delta
            blocks[z * 2 + core, m * rows + at:m * rows + end, :] = whole.astype(jnp.bfloat16)

    started = []

    def go(copy):
        copy.start()
        started.append(copy)

    def first_way(k):
        maybe(z > 0, lambda: l_copy(0, k).start())
        maybe(z == 0, lambda: r_copy(0, k).start())

    def second_way(k):
        maybe(z > 0, lambda: r_copy(0, k).start())
        maybe(z == 0, lambda: l_copy(0, k).start())

    def own_sent(k):
        started.append(r_copy(0, k))
        started.append(l_copy(0, k))

    def compute_all(at, end):
        for k in range(at, end):
            compute(k)
            if k == at:
                continue
            yield k - 1
        yield end - 1

    lead = LEAD
    for n, k in enumerate(compute_all(0, lead)):
        if n == 0:
            greeted()
            maybe(z == 0, lambda: pl.semaphore_wait(right_in, 1))
        first_way(k)
    maybe(jnp.logical_and(z > 0, z < NZ - 1), lambda: pl.semaphore_wait(right_in, 1))
    maybe(z == 0, lambda: pl.semaphore_wait(left_in, 1))
    for k in range(lead):
        second_way(k)
    def own_sib(k):
        own_sent(k)
        go(s_copy(0, k))

    for k in compute_all(lead, len(PIECES[0])):
        if k < NORM_AT:
            first_way(k)
            second_way(k)
    maybe(core == 1, lambda: pl.semaphore_wait(sib_in, 1))
    for k in range(NORM_AT):
        own_sib(k)

    for copy in norm_loads:
        copy.wait()
    gain = (nt_v[...] + ns_v[...]).astype(jnp.bfloat16)
    t = y * NX + x
    lane = lax.broadcasted_iota(jnp.int32, (16, 128), 1)
    entry = lax.broadcasted_iota(jnp.int32, (16, 128), 0)
    place = jnp.where(lane == lax.rem(t, 8) * 16 + entry, 1.0, 0.0).astype(jnp.bfloat16)
    spread = jnp.dot(jnp.broadcast_to(gain, (16, 16)), place, preferred_element_type=jnp.float32)[:8]
    row = lax.broadcasted_iota(jnp.int32, (8, 128), 0)
    nx[x] = jnp.where(row == core * 2 + t // 8, spread, 0.0)

    def spread_over(buf, at, size, axis, send, recv):
        copies = []
        for k in range(1, size):
            device = {axis: lax.rem(at + k, size)}
            copies.append(remote(buf.at[at], buf.at[at], send.at[k - 1], recv.at[k - 1], device))
            go(copies[-1])
        for k in range(1, size):
            source = lax.rem(at + size - k, size)
            remote(buf.at[source], buf.at[source], send.at[k - 1], recv.at[k - 1], {axis: source}).wait_recv()

    maybe(x < NX - 1, lambda: pl.semaphore_wait(x_in, NX - 1 - x))
    maybe(y < NY - 1, lambda: pl.semaphore_wait(y_in, NY - 1 - y))
    spread_over(nx, x, NX, "x", nxs, nxr)
    ny[y] = nx[0] + nx[1] + nx[2] + nx[3]
    spread_over(ny, y, NY, "y", nys, nyr)
    ncore[core] = ny[0] + ny[1] + ny[2] + ny[3]
    go(remote(ncore.at[core], ncore.at[core], nss, nsr, sib))
    remote(ncore.at[1 - core], ncore.at[1 - core], nss, nsr, sib).wait_recv()
    nz[z] = (ncore[0] + ncore[1]).astype(jnp.bfloat16)

    def norm_r(step):
        at = nz.at[lax.rem(z + NZ - step, NZ)]
        return remote(at, at, nrs.at[step], nrr.at[step], right)

    def norm_l(step):
        at = nz.at[lax.rem(z + step, NZ)]
        return remote(at, at, nls.at[step], nlr.at[step], left)

    def norm_step(step):
        at = nz.at[lax.rem(z + NZ - step - 1, NZ)]
        remote(at, at, nrs.at[step], nrr.at[step], right).wait_recv()
        if step < 3:
            go(norm_r(step + 1))
            at = nz.at[lax.rem(z + step + 1, NZ)]
            remote(at, at, nls.at[step], nlr.at[step], left).wait_recv()
            if step < 2:
                go(norm_l(step + 1))

    go(norm_r(0))
    go(norm_l(0))
    for k in range(NORM_AT, len(PIECES[0])):
        first_way(k)
        second_way(k)
        own_sib(k)

    parted = []

    def part(cond, copy):
        maybe(cond, copy.start)
        parted.append((cond, copy))

    def inside(piece, held):
        return all(any(r0 <= row < r0 + n for r0, n in held) for row in range(piece[0], piece[0] + piece[1], 4))

    for step in range(3):
        after = PIECES[step + 1]
        waiting = [list(range(len(after))), list(range(len(after)))]
        for k, piece in enumerate(PIECES[step]):
            if k == min(NORM_AT, len(PIECES[step]) - 1):
                norm_step(step)
            for way, (wait, copy, dist) in enumerate(((r_wait, r_copy, NZ - step - 1), (l_wait, l_copy, step + 1))):
                wait(step, k)
                while waiting[way] and inside(after[waiting[way][0]], PIECES[step][:k + 1]):
                    p = waiting[way].pop(0)
                    if step < 2:
                        go(copy(step + 1, p))
                    elif (p < low) if way == 0 else (p >= high):
                        go(copy(step + 1, p))
                    elif low <= p < high:
                        part(p < r_out if way == 0 else p >= l_out, copy(step + 1, p))
                go(s_copy(dist, k))

    for k in [v for pair in zip(range(count // 2), range(count // 2, count)) for v in pair]:
        if k < low:
            r_wait(3, k)
        elif k >= high:
            l_wait(3, k)
        else:
            maybe(k < r_in, lambda: r_wait(3, k))
            maybe(k >= l_in, lambda: l_wait(3, k))
        go(s_copy(4, k))

    norm_step(3)
    for k in range(NZ):
        nrow[4 * k:4 * k + 4, :] = nz[k, 0:4, :].astype(jnp.float32)
    onorm[...] = nrow[...].astype(jnp.bfloat16)

    for copy in started:
        copy.wait_send()
    for cond, copy in parted:
        maybe(cond, copy.wait_send)
    for dist in range(NZ):
        for k in range(len(PIECES[table(dist)])):
            s_wait(dist, k)


def gathered(*args):
    w, a, b, norms = args[0:3], args[3:6], args[6:9], args[9:11]
    rows, width = w[0].shape
    rank = a[0].shape[0]
    whole = pltpu.VMEM((16, 3 * rows, width), jnp.bfloat16)
    vmem = pl.BlockSpec(memory_space=pltpu.VMEM)
    hbm = pl.BlockSpec(memory_space=pltpu.HBM)
    dma = pltpu.SemaphoreType.DMA
    regular = pltpu.SemaphoreType.REGULAR
    f32 = jnp.float32
    return pl.pallas_call(
        functools.partial(body, rows),
        out_shape=(whole, pltpu.VMEM((32, 128), jnp.bfloat16)),
        in_specs=[hbm] * 11,
        out_specs=(vmem,) * 2,
        scratch_shapes=[
            pltpu.VMEM((3, rows, width), jnp.bfloat16),
            pltpu.VMEM((3, rank, rows), jnp.bfloat16),
            pltpu.VMEM((3, rank, width), jnp.bfloat16),
            pltpu.VMEM((1, 16), f32),
            pltpu.VMEM((1, 16), f32),
            pltpu.VMEM((8, 8, 128), jnp.bfloat16),
            pltpu.VMEM((2, 8, 128), f32),
            pltpu.VMEM((4, 8, 128), f32),
            pltpu.VMEM((4, 8, 128), f32),
            pltpu.VMEM((32, 128), f32),
            dma((4, 3)),
            dma((4, MOST)), dma((4, MOST)), dma((8, MOST)),
            dma((4, MOST)), dma((4, MOST)), dma((8, MOST)),
            dma((4,)), dma((4,)), dma((4,)), dma((4,)),
            dma, dma, dma((3,)), dma((3,)), dma((3,)), dma((3,)),
            regular, regular, regular, regular, regular,
        ],
        compiler_params=pltpu.CompilerParams(collective_id=0, has_side_effects=True, vmem_limit_bytes=30 * 2**20),
        name="merge_and_gather",
    )(*[pltpu.with_memory_space_constraint(v, pltpu.HBM) for v in (*w, *a, *b, *norms)])


def write_out(blocks, row, gate, up, down, norm, sems):
    rows, width = gate.shape[0], blocks.shape[2]
    copies = [pltpu.make_async_copy(row, norm, sems.at[3, 0])]
    for m, out in enumerate((gate, up, down)):
        for f in range(blocks.shape[0]):
            copies.append(pltpu.make_async_copy(
                blocks.at[f, pl.ds(m * rows, rows), :], out.at[:, pl.ds(f * width, width)], sems.at[m, f]))
    for copy in copies:
        copy.start()
    for copy in copies:
        copy.wait()


def written(blocks, row):
    count, rows, width = blocks.shape
    whole = jax.ShapeDtypeStruct((rows // 3, count * width), blocks.dtype)
    return pl.pallas_call(
        write_out,
        out_shape=(whole, whole, whole, jax.ShapeDtypeStruct(row.shape, row.dtype)),
        in_specs=[pl.BlockSpec(memory_space=pltpu.VMEM)] * 2,
        out_specs=(pl.BlockSpec(memory_space=pltpu.HBM),) * 4,
        scratch_shapes=[pltpu.SemaphoreType.DMA((4, count))],
        compiler_params=pltpu.CompilerParams(vmem_limit_bytes=2**20),
        name="write_out",
    )(blocks, row)


def local(w_gate, low_gate, high_gate, w_up, low_up, high_up, w_down, low_down, high_down, norm_train, norm_step):
    blocks, row = gathered(
        w_gate.T, w_up.T, w_down, high_gate, high_up, low_down.T, low_gate.T, low_up.T, high_down,
        norm_train.reshape(1, 16), norm_step.reshape(1, 16))
    gate, up, down, norm = written(blocks, row)
    return gate.T, up.T, down, norm.reshape(-1)


def solution(mesh):
    finer = Mesh(mesh.devices.reshape(8, 2, 4, 4), AXES)
    in_specs = (
        P(FSDP, TP), P(FSDP, None), P(None, TP),
        P(FSDP, TP), P(FSDP, None), P(None, TP),
        P(TP, FSDP), P(TP, None), P(None, FSDP),
        P(FSDP + TP), P(FSDP + TP),
    )
    out_specs = (P(None, TP), P(None, TP), P(TP, None), P())
    return jax.shard_map(local, mesh=finer, in_specs=in_specs, out_specs=out_specs, check_vma=False)
```

```python
import functools

import jax
import jax.numpy as jnp
from jax import lax
from jax.experimental import pallas as pl
from jax.experimental.pallas import tpu as pltpu
from jax.sharding import Mesh
from jax.sharding import PartitionSpec as P

mix_rate = 2.0
SHIFT = 1
LEAD = 2
MESH = pl.DeviceIdType.MESH
AXES = ("z", "core", "y", "x")
FSDP = ("z", "core")
TP = ("y", "x")
NZ, NX, NY = 8, 4, 4
PIECES = (((0, 88), (88, 432), (520, 512), (1032, 520), (1552, 512)), ((0, 520), (520, 512), (1032, 520), (1552, 512)), ((0, 520), (520, 512), (1032, 520), (1552, 512)), ((0, 520), (520, 256), (776, 256), (1032, 256), (1288, 256), (1544, 520)))
MOST = max(len(p) for p in PIECES)


def body(rows, *refs):
    (wg, wu, wd, ag, au, ad, bg, bu, bd, ntrain, nstep, blocks, onorm,
     w_v, a_v, b_v, nt_v, ns_v, nz, ncore, nx, ny, nrow,
     in_sem, r_recv, l_recv, s_recv, r_send, l_send, s_send,
     nzr, nzs, nsr, nss, nxr, nxs, nyr, nys,
     right_in, left_in, z_in, x_in, y_in, sib_in) = refs
    w_hbm, a_hbm, b_hbm = (wg, wu, wd), (ag, au, ad), (bg, bu, bd)
    z, core, y, x = (lax.axis_index(k) for k in AXES)
    right, left = {"z": lax.rem(z + 1, NZ)}, {"z": lax.rem(z + NZ - 1, NZ)}
    sib = {"core": 1 - core}

    barrier = pltpu.get_barrier_semaphore()

    def maybe(cond, act):
        @pl.when(cond)
        def _():
            act()

    def signal(sem, device):
        pl.semaphore_signal(sem, inc=1, device_id=device, device_id_type=MESH)

    for k in range(1, NZ):
        maybe(z + k < NZ, lambda: signal(barrier, {"z": z + k}))

    @pl.when(core == 1)
    def _():
        signal(barrier, sib)

    loads = []
    for m in range(3):
        loads.append([
            pltpu.make_async_copy(w_hbm[m], w_v.at[m], in_sem.at[m, 0]),
            pltpu.make_async_copy(a_hbm[m], a_v.at[m], in_sem.at[m, 1]),
            pltpu.make_async_copy(b_hbm[m], b_v.at[m], in_sem.at[m, 2]),
        ])
    norm_loads = [
        pltpu.make_async_copy(ntrain, nt_v, in_sem.at[3, 0]),
        pltpu.make_async_copy(nstep, ns_v, in_sem.at[3, 1]),
    ]
    for m in range(3):
        for copy in loads[m]:
            copy.start()
    for copy in norm_loads:
        copy.start()
    for k in range(1, NX):
        maybe(x + k < NX, lambda: signal(barrier, {"x": x + k}))
    for k in range(1, NY):
        maybe(y + k < NY, lambda: signal(barrier, {"y": y + k}))

    def greeted():
        greetings = x + y + z + (1 - core)
        maybe(greetings > 0, lambda: pl.semaphore_wait(barrier, greetings))

        @pl.when(z > 0)
        def _():
            signal(right_in, left)

        @pl.when(z == NZ - 1)
        def _():
            signal(left_in, right)

        @pl.when(core == 0)
        def _():
            signal(sib_in, sib)

        for k in range(1, NZ):
            maybe(z - k >= 0, lambda: signal(z_in, {"z": z - k}))
        for k in range(1, NX):
            maybe(x - k >= 0, lambda: signal(x_in, {"x": x - k}))
        for k in range(1, NY):
            maybe(y - k >= 0, lambda: signal(y_in, {"y": y - k}))

    def spot(step, k, block_z, block_core):
        r0, n = PIECES[step][k]
        return blocks.at[block_z * 2 + block_core, pl.ds(r0, n), :]

    def remote(src, dst, send, recv, device):
        return pltpu.make_async_remote_copy(
            src_ref=src, dst_ref=dst, send_sem=send, recv_sem=recv, device_id=device, device_id_type=MESH)

    count = len(PIECES[3])

    def split(at):
        return count // 2 + jnp.where(at == NZ - 1, SHIFT, 0) - jnp.where(at == 0, SHIFT, 0)

    r_out, r_in = split(lax.rem(z + 1, NZ)), split(z)
    l_out, l_in = split(lax.rem(z + NZ - 1, NZ)), split(z)
    low, high = count // 2 - SHIFT, count // 2 + SHIFT

    def r_copy(step, k):
        at = spot(step, k, lax.rem(z + NZ - step, NZ), core)
        return remote(at, at, r_send.at[step, k], r_recv.at[step, k], right)

    def l_copy(step, k):
        at = spot(step, k, lax.rem(z + step, NZ), core)
        return remote(at, at, l_send.at[step, k], l_recv.at[step, k], left)

    def r_wait(step, k):
        at = spot(step, k, lax.rem(z + NZ - step - 1, NZ), core)
        remote(at, at, r_send.at[step, k], r_recv.at[step, k], right).wait_recv()

    def l_wait(step, k):
        at = spot(step, k, lax.rem(z + step + 1, NZ), core)
        remote(at, at, l_send.at[step, k], l_recv.at[step, k], left).wait_recv()

    def table(dist):
        return max(min(dist, NZ - dist) - 1, 0)

    def s_copy(dist, k):
        at = spot(table(dist), k, lax.rem(z + dist, NZ), core)
        return remote(at, at, s_send.at[dist, k], s_recv.at[dist, k], sib)

    def s_wait(dist, k):
        at = spot(table(dist), k, lax.rem(z + dist, NZ), 1 - core)
        remote(at, at, s_send.at[dist, k], s_recv.at[dist, k], sib).wait_recv()

    loaded = set()

    def compute(k):
        r0, n = PIECES[0][k]
        for m in range(3):
            at, end = max(r0, m * rows) - m * rows, min(r0 + n, (m + 1) * rows) - m * rows
            if at >= end:
                continue
            if m not in loaded:
                loaded.add(m)
                for copy in loads[m]:
                    copy.wait()
            delta = lax.dot_general(
                a_v[m, :, at:end], b_v[m], (((0,), (0,)), ((), ())), preferred_element_type=jnp.float32)
            whole = w_v[m, at:end, :].astype(jnp.float32) + mix_rate * delta
            blocks[z * 2 + core, m * rows + at:m * rows + end, :] = whole.astype(jnp.bfloat16)

    started = []

    def go(copy):
        copy.start()
        started.append(copy)

    def first_way(k):
        maybe(z > 0, lambda: l_copy(0, k).start())
        maybe(z == 0, lambda: r_copy(0, k).start())

    def second_way(k):
        maybe(z > 0, lambda: r_copy(0, k).start())
        maybe(z == 0, lambda: l_copy(0, k).start())

    def own_sent(k):
        started.append(r_copy(0, k))
        started.append(l_copy(0, k))

    def compute_all(at, end):
        for k in range(at, end):
            compute(k)
            if k == at:
                continue
            yield k - 1
        yield end - 1

    lead = LEAD
    greeted()
    for n, k in enumerate(compute_all(0, lead)):
        if n == 0:
            maybe(z == 0, lambda: pl.semaphore_wait(right_in, 1))
        first_way(k)
    maybe(jnp.logical_and(z > 0, z < NZ - 1), lambda: pl.semaphore_wait(right_in, 1))
    maybe(z == 0, lambda: pl.semaphore_wait(left_in, 1))
    for k in range(lead):
        second_way(k)

    def own_sib(k):
        own_sent(k)
        go(s_copy(0, k))

    for k in compute_all(lead, len(PIECES[0])):
        first_way(k)
        second_way(k)
    maybe(core == 1, lambda: pl.semaphore_wait(sib_in, 1))
    for k in range(len(PIECES[0])):
        own_sib(k)

    for copy in norm_loads:
        copy.wait()
    gain = (nt_v[...] + ns_v[...]).astype(jnp.bfloat16)
    t = y * NX + x
    lane = lax.broadcasted_iota(jnp.int32, (16, 128), 1)
    entry = lax.broadcasted_iota(jnp.int32, (16, 128), 0)
    place = jnp.where(lane == lax.rem(t, 8) * 16 + entry, 1.0, 0.0).astype(jnp.bfloat16)
    spread = jnp.dot(jnp.broadcast_to(gain, (16, 16)), place, preferred_element_type=jnp.float32)[:8]
    row = lax.broadcasted_iota(jnp.int32, (8, 128), 0)
    nx[x] = jnp.where(row == core * 2 + t // 8, spread, 0.0)

    def spread_over(buf, at, size, axis, send, recv):
        for k in range(1, size):
            device = {axis: lax.rem(at + k, size)}
            go(remote(buf.at[at], buf.at[at], send.at[k - 1], recv.at[k - 1], device))

    def collect(buf, at, size, axis, send, recv):
        for k in range(1, size):
            source = lax.rem(at + size - k, size)
            remote(buf.at[source], buf.at[source], send.at[k - 1], recv.at[k - 1], {axis: source}).wait_recv()

    maybe(x < NX - 1, lambda: pl.semaphore_wait(x_in, NX - 1 - x))
    maybe(y < NY - 1, lambda: pl.semaphore_wait(y_in, NY - 1 - y))
    spread_over(nx, x, NX, "x", nxs, nxr)
    collect(nx, x, NX, "x", nxs, nxr)
    ny[y] = nx[0] + nx[1] + nx[2] + nx[3]
    spread_over(ny, y, NY, "y", nys, nyr)
    collect(ny, y, NY, "y", nys, nyr)
    ncore[core] = ny[0] + ny[1] + ny[2] + ny[3]
    go(remote(ncore.at[core], ncore.at[core], nss, nsr, sib))
    remote(ncore.at[1 - core], ncore.at[1 - core], nss, nsr, sib).wait_recv()
    nz[z] = (ncore[0] + ncore[1])[0:4].astype(jnp.bfloat16)

    maybe(z < NZ - 1, lambda: pl.semaphore_wait(z_in, NZ - 1 - z))
    spread_over(nz, z, NZ, "z", nzs, nzr)

    parted = []

    def part(cond, copy):
        maybe(cond, copy.start)
        parted.append((cond, copy))

    def inside(piece, held):
        return all(any(r0 <= row < r0 + n for r0, n in held) for row in range(piece[0], piece[0] + piece[1], 4))

    for step in range(3):
        after = PIECES[step + 1]
        waiting = [list(range(len(after))), list(range(len(after)))]
        if step == 2:
            waiting = [list(range(high)), [*range(high, count), *reversed(range(low, high))]]
        for k, piece in enumerate(PIECES[step]):
            for way, (wait, copy, dist) in enumerate(((r_wait, r_copy, NZ - step - 1), (l_wait, l_copy, step + 1))):
                wait(step, k)
                while waiting[way] and inside(after[waiting[way][0]], PIECES[step][:k + 1]):
                    p = waiting[way].pop(0)
                    if step < 2:
                        go(copy(step + 1, p))
                    elif (p < low) if way == 0 else (p >= high):
                        go(copy(step + 1, p))
                    elif low <= p < high:
                        part(p < r_out if way == 0 else p >= l_out, copy(step + 1, p))
                go(s_copy(dist, k))

    for k in [v for pair in zip(range(low), range(high, count)) for v in pair] + list(range(low, high)):
        if k < low:
            r_wait(3, k)
        elif k >= high:
            l_wait(3, k)
        else:
            maybe(k < r_in, lambda: r_wait(3, k))
            maybe(k >= l_in, lambda: l_wait(3, k))
        go(s_copy(4, k))

    collect(nz, z, NZ, "z", nzs, nzr)
    for k in range(NZ):
        nrow[4 * k:4 * k + 4, :] = nz[k].astype(jnp.float32)
    onorm[...] = nrow[...].astype(jnp.bfloat16)

    for copy in started:
        copy.wait_send()
    for cond, copy in parted:
        maybe(cond, copy.wait_send)
    for dist in range(NZ):
        for k in range(len(PIECES[table(dist)])):
            s_wait(dist, k)


def gathered(*args):
    w, a, b, norms = args[0:3], args[3:6], args[6:9], args[9:11]
    rows, width = w[0].shape
    rank = a[0].shape[0]
    whole = pltpu.VMEM((16, 3 * rows, width), jnp.bfloat16)
    vmem = pl.BlockSpec(memory_space=pltpu.VMEM)
    hbm = pl.BlockSpec(memory_space=pltpu.HBM)
    dma = pltpu.SemaphoreType.DMA
    regular = pltpu.SemaphoreType.REGULAR
    f32 = jnp.float32
    return pl.pallas_call(
        functools.partial(body, rows),
        out_shape=(whole, pltpu.VMEM((32, 128), jnp.bfloat16)),
        in_specs=[hbm] * 11,
        out_specs=(vmem,) * 2,
        scratch_shapes=[
            pltpu.VMEM((3, rows, width), jnp.bfloat16),
            pltpu.VMEM((3, rank, rows), jnp.bfloat16),
            pltpu.VMEM((3, rank, width), jnp.bfloat16),
            pltpu.VMEM((1, 16), f32),
            pltpu.VMEM((1, 16), f32),
            pltpu.VMEM((8, 4, 128), jnp.bfloat16),
            pltpu.VMEM((2, 8, 128), f32),
            pltpu.VMEM((4, 8, 128), f32),
            pltpu.VMEM((4, 8, 128), f32),
            pltpu.VMEM((32, 128), f32),
            dma((4, 3)),
            dma((4, MOST)), dma((4, MOST)), dma((8, MOST)),
            dma((4, MOST)), dma((4, MOST)), dma((8, MOST)),
            dma((7,)), dma((7,)), dma, dma, dma((3,)), dma((3,)), dma((3,)), dma((3,)),
            regular, regular, regular, regular, regular, regular,
        ],
        compiler_params=pltpu.CompilerParams(collective_id=0, has_side_effects=True, vmem_limit_bytes=30 * 2**20),
        name="merge_and_gather",
    )(*[pltpu.with_memory_space_constraint(v, pltpu.HBM) for v in (*w, *a, *b, *norms)])


def write_out(blocks, row, gate, up, down, norm, sems):
    rows, width = gate.shape[0], blocks.shape[2]
    copies = [pltpu.make_async_copy(row, norm, sems.at[3, 0])]
    for f in range(blocks.shape[0]):
        for m, out in enumerate((gate, up, down)):
            copies.append(pltpu.make_async_copy(
                blocks.at[f, pl.ds(m * rows, rows), :], out.at[:, pl.ds(f * width, width)], sems.at[m, f]))
    for copy in copies:
        copy.start()
    for copy in copies:
        copy.wait()


def written(blocks, row):
    count, rows, width = blocks.shape
    whole = jax.ShapeDtypeStruct((rows // 3, count * width), blocks.dtype)
    return pl.pallas_call(
        write_out,
        out_shape=(whole, whole, whole, jax.ShapeDtypeStruct(row.shape, row.dtype)),
        in_specs=[pl.BlockSpec(memory_space=pltpu.VMEM)] * 2,
        out_specs=(pl.BlockSpec(memory_space=pltpu.HBM),) * 4,
        scratch_shapes=[pltpu.SemaphoreType.DMA((4, count))],
        compiler_params=pltpu.CompilerParams(vmem_limit_bytes=2**20),
        name="write_out",
    )(blocks, row)


def local(w_gate, low_gate, high_gate, w_up, low_up, high_up, w_down, low_down, high_down, norm_train, norm_step):
    blocks, row = gathered(
        w_gate.T, w_up.T, w_down, high_gate, high_up, low_down.T, low_gate.T, low_up.T, high_down,
        norm_train.reshape(1, 16), norm_step.reshape(1, 16))
    gate, up, down, norm = written(blocks, row)
    return gate.T, up.T, down, norm.reshape(-1)


def solution(mesh):
    finer = Mesh(mesh.devices.reshape(8, 2, 4, 4), AXES)
    in_specs = (
        P(FSDP, TP), P(FSDP, None), P(None, TP),
        P(FSDP, TP), P(FSDP, None), P(None, TP),
        P(TP, FSDP), P(TP, None), P(None, FSDP),
        P(FSDP + TP), P(FSDP + TP),
    )
    out_specs = (P(None, TP), P(None, TP), P(TP, None), P())
    return jax.shard_map(local, mesh=finer, in_specs=in_specs, out_specs=out_specs, check_vma=False)
```

```python
import functools

import jax
import jax.numpy as jnp
from jax import lax
from jax.experimental import pallas as pl
from jax.experimental.pallas import tpu as pltpu
from jax.sharding import Mesh
from jax.sharding import PartitionSpec as P

mix_rate = 2.0
SHIFT = 1
LEAD = 2
MESH = pl.DeviceIdType.MESH
AXES = ("z", "core", "y", "x")
FSDP = ("z", "core")
TP = ("y", "x")
NZ, NX, NY = 8, 4, 4
PIECES = (((0, 88), (88, 432), (520, 512), (1032, 520), (1552, 512)), ((0, 520), (520, 512), (1032, 520), (1552, 512)), ((0, 520), (520, 512), (1032, 520), (1552, 512)), ((0, 520), (520, 280), (800, 232), (1032, 200), (1232, 312), (1544, 520)))


def flat(step, k):
    return sum(len(p) for p in PIECES[:step]) + k


def table(dist):
    return max(min(dist, NZ - dist) - 1, 0)


def flat_sib(dist, k):
    return sum(len(PIECES[table(d)]) for d in range(dist)) + k


def body(rows, *refs):
    (wg, wu, wd, ag, au, ad, bg, bu, bd, ntrain, nstep, blocks, onorm,
     w_v, a_v, b_v, nt_v, ns_v, nz, ncore, nx, ny, nrow,
     in_sem, r_recv, l_recv, s_recv, r_send, l_send, s_send,
     nzr, nzs, nsr, nss, nxr, nxs, nyr, nys,
     right_in, left_in, z_in, x_in, y_in, sib_in) = refs
    w_hbm, a_hbm, b_hbm = (wg, wu, wd), (ag, au, ad), (bg, bu, bd)
    z, core, y, x = (lax.axis_index(k) for k in AXES)
    right, left = {"z": lax.rem(z + 1, NZ)}, {"z": lax.rem(z + NZ - 1, NZ)}
    sib = {"core": 1 - core}

    barrier = pltpu.get_barrier_semaphore()

    def maybe(cond, act):
        @pl.when(cond)
        def _():
            act()

    def signal(sem, device):
        pl.semaphore_signal(sem, inc=1, device_id=device, device_id_type=MESH)

    for k in range(1, NZ):
        maybe(z + k < NZ, lambda: signal(barrier, {"z": z + k}))

    @pl.when(core == 1)
    def _():
        signal(barrier, sib)

    loads = []
    for m in range(3):
        loads.append([
            pltpu.make_async_copy(w_hbm[m], w_v.at[m], in_sem.at[m, 0]),
            pltpu.make_async_copy(a_hbm[m], a_v.at[m], in_sem.at[m, 1]),
            pltpu.make_async_copy(b_hbm[m], b_v.at[m], in_sem.at[m, 2]),
        ])
    norm_loads = [
        pltpu.make_async_copy(ntrain, nt_v, in_sem.at[3, 0]),
        pltpu.make_async_copy(nstep, ns_v, in_sem.at[3, 1]),
    ]
    for m in range(3):
        for copy in loads[m]:
            copy.start()
    for copy in norm_loads:
        copy.start()
    for k in range(1, NX):
        maybe(x + k < NX, lambda: signal(barrier, {"x": x + k}))
    for k in range(1, NY):
        maybe(y + k < NY, lambda: signal(barrier, {"y": y + k}))

    def greeted():
        greetings = x + y + z + (1 - core)
        maybe(greetings > 0, lambda: pl.semaphore_wait(barrier, greetings))

        @pl.when(z > 0)
        def _():
            signal(right_in, left)

        @pl.when(z == NZ - 1)
        def _():
            signal(left_in, right)

        @pl.when(core == 0)
        def _():
            signal(sib_in, sib)

        for k in range(1, NZ):
            maybe(z - k >= 0, lambda: signal(z_in, {"z": z - k}))
        for k in range(1, NX):
            maybe(x - k >= 0, lambda: signal(x_in, {"x": x - k}))
        for k in range(1, NY):
            maybe(y - k >= 0, lambda: signal(y_in, {"y": y - k}))

    def spot(step, k, block_z, block_core):
        r0, n = PIECES[step][k]
        return blocks.at[block_z * 2 + block_core, pl.ds(r0, n), :]

    def remote(src, dst, send, recv, device):
        return pltpu.make_async_remote_copy(
            src_ref=src, dst_ref=dst, send_sem=send, recv_sem=recv, device_id=device, device_id_type=MESH)

    count = len(PIECES[3])

    def split(at):
        return count // 2 + jnp.where(at == NZ - 1, SHIFT, 0) - jnp.where(at == 0, SHIFT, 0)

    r_out, r_in = split(lax.rem(z + 1, NZ)), split(z)
    l_out, l_in = split(lax.rem(z + NZ - 1, NZ)), split(z)
    low, high = count // 2 - SHIFT, count // 2 + SHIFT

    def r_copy(step, k):
        at = spot(step, k, lax.rem(z + NZ - step, NZ), core)
        return remote(at, at, r_send.at[1 + k if step == 3 else 0], r_recv.at[flat(step, k)], right)

    def l_copy(step, k):
        at = spot(step, k, lax.rem(z + step, NZ), core)
        return remote(at, at, l_send.at[1 + k if step == 3 else 0], l_recv.at[flat(step, k)], left)

    def r_wait(step, k):
        at = spot(step, k, lax.rem(z + NZ - step - 1, NZ), core)
        remote(at, at, r_send.at[0], r_recv.at[flat(step, k)], right).wait_recv()

    def l_wait(step, k):
        at = spot(step, k, lax.rem(z + step + 1, NZ), core)
        remote(at, at, l_send.at[0], l_recv.at[flat(step, k)], left).wait_recv()

    def s_copy(dist, k):
        at = spot(table(dist), k, lax.rem(z + dist, NZ), core)
        return remote(at, at, s_send.at[0], s_recv.at[flat_sib(dist, k)], sib)

    def s_wait(dist, k):
        at = spot(table(dist), k, lax.rem(z + dist, NZ), 1 - core)
        remote(at, at, s_send.at[0], s_recv.at[flat_sib(dist, k)], sib).wait_recv()

    loaded = set()

    def compute(k):
        r0, n = PIECES[0][k]
        for m in range(3):
            at, end = max(r0, m * rows) - m * rows, min(r0 + n, (m + 1) * rows) - m * rows
            if at >= end:
                continue
            if m not in loaded:
                loaded.add(m)
                for copy in loads[m]:
                    copy.wait()
            delta = lax.dot_general(
                a_v[m, :, at:end], b_v[m], (((0,), (0,)), ((), ())), preferred_element_type=jnp.float32)
            whole = w_v[m, at:end, :].astype(jnp.float32) + mix_rate * delta
            blocks[z * 2 + core, m * rows + at:m * rows + end, :] = whole.astype(jnp.bfloat16)

    started = []

    def go(copy):
        copy.start()
        started.append(copy)

    def first_way(k):
        maybe(z > 0, lambda: l_copy(0, k).start())
        maybe(z == 0, lambda: r_copy(0, k).start())

    def second_way(k):
        maybe(z > 0, lambda: r_copy(0, k).start())
        maybe(z == 0, lambda: l_copy(0, k).start())

    def compute_all(at, end):
        for k in range(at, end):
            compute(k)
            if k == at:
                continue
            yield k - 1
        yield end - 1

    lead = LEAD
    greeted()
    for n, k in enumerate(compute_all(0, lead)):
        if n == 0:
            maybe(z == 0, lambda: pl.semaphore_wait(right_in, 1))
        first_way(k)
    maybe(jnp.logical_and(z > 0, z < NZ - 1), lambda: pl.semaphore_wait(right_in, 1))
    maybe(z == 0, lambda: pl.semaphore_wait(left_in, 1))
    for k in range(lead):
        second_way(k)

    def own_sib(k):
        s_copy(0, k).start()

    for k in compute_all(lead, len(PIECES[0])):
        first_way(k)
        second_way(k)
    maybe(core == 1, lambda: pl.semaphore_wait(sib_in, 1))
    for k in range(len(PIECES[0])):
        own_sib(k)

    for copy in norm_loads:
        copy.wait()
    gain = (nt_v[...] + ns_v[...]).astype(jnp.bfloat16)
    t = y * NX + x
    lane = lax.broadcasted_iota(jnp.int32, (16, 128), 1)
    entry = lax.broadcasted_iota(jnp.int32, (16, 128), 0)
    place = jnp.where(lane == lax.rem(t, 8) * 16 + entry, 1.0, 0.0).astype(jnp.bfloat16)
    spread = jnp.dot(jnp.broadcast_to(gain, (16, 16)), place, preferred_element_type=jnp.float32)[:8]
    row = lax.broadcasted_iota(jnp.int32, (8, 128), 0)
    nx[x] = jnp.where(row == core * 2 + t // 8, spread, 0.0)

    def spread_over(buf, at, size, axis, send, recv):
        for k in range(1, size):
            device = {axis: lax.rem(at + k, size)}
            go(remote(buf.at[at], buf.at[at], send.at[k - 1], recv.at[k - 1], device))

    def collect(buf, at, size, axis, send, recv):
        for k in range(1, size):
            source = lax.rem(at + size - k, size)
            remote(buf.at[source], buf.at[source], send.at[k - 1], recv.at[k - 1], {axis: source}).wait_recv()

    maybe(x < NX - 1, lambda: pl.semaphore_wait(x_in, NX - 1 - x))
    maybe(y < NY - 1, lambda: pl.semaphore_wait(y_in, NY - 1 - y))
    spread_over(nx, x, NX, "x", nxs, nxr)
    collect(nx, x, NX, "x", nxs, nxr)
    ny[y] = nx[0] + nx[1] + nx[2] + nx[3]
    spread_over(ny, y, NY, "y", nys, nyr)
    collect(ny, y, NY, "y", nys, nyr)
    ncore[core] = ny[0] + ny[1] + ny[2] + ny[3]
    go(remote(ncore.at[core], ncore.at[core], nss, nsr, sib))
    remote(ncore.at[1 - core], ncore.at[1 - core], nss, nsr, sib).wait_recv()
    nz[z] = (ncore[0] + ncore[1])[0:4].astype(jnp.bfloat16)

    maybe(z < NZ - 1, lambda: pl.semaphore_wait(z_in, NZ - 1 - z))
    spread_over(nz, z, NZ, "z", nzs, nzr)

    parted = []

    def part(cond, copy):
        maybe(cond, copy.start)
        parted.append((cond, copy))

    def inside(piece, held):
        return all(any(r0 <= row < r0 + n for r0, n in held) for row in range(piece[0], piece[0] + piece[1], 4))

    for step in range(3):
        after = PIECES[step + 1]
        waiting = [list(range(len(after))), list(range(len(after)))]
        if step == 2:
            waiting = [list(range(high)), [*range(high, count), *reversed(range(low, high))]]
        for k, piece in enumerate(PIECES[step]):
            for way, (wait, copy, dist) in enumerate(((r_wait, r_copy, NZ - step - 1), (l_wait, l_copy, step + 1))):
                wait(step, k)
                while waiting[way] and inside(after[waiting[way][0]], PIECES[step][:k + 1]):
                    p = waiting[way].pop(0)
                    if step < 2:
                        copy(step + 1, p).start()
                    elif (p < low) if way == 0 else (p >= high):
                        go(copy(step + 1, p))
                    elif low <= p < high:
                        part(p < r_out if way == 0 else p >= l_out, copy(step + 1, p))
                s_copy(dist, k).start()

    for k in [v for pair in zip(range(low), range(high, count)) for v in pair] + list(range(low, high)):
        if k < low:
            r_wait(3, k)
        elif k >= high:
            l_wait(3, k)
        else:
            maybe(k < r_in, lambda: r_wait(3, k))
            maybe(k >= l_in, lambda: l_wait(3, k))
        s_copy(4, k).start()

    collect(nz, z, NZ, "z", nzs, nzr)
    for k in range(NZ):
        nrow[4 * k:4 * k + 4, :] = nz[k].astype(jnp.float32)
    onorm[...] = nrow[...].astype(jnp.bfloat16)

    for count, sem in ((3, r_send), (3, l_send), (NZ, s_send)):
        sent = blocks.at[pl.ds(0, count)]
        remote(sent, sent, sem.at[0], r_recv.at[0], right).wait_send()
    for copy in started:
        copy.wait_send()
    for cond, copy in parted:
        maybe(cond, copy.wait_send)
    for dist in range(NZ):
        for k in range(len(PIECES[table(dist)])):
            s_wait(dist, k)


def gathered(*args):
    w, a, b, norms = args[0:3], args[3:6], args[6:9], args[9:11]
    rows, width = w[0].shape
    rank = a[0].shape[0]
    whole = pltpu.VMEM((16, 3 * rows, width), jnp.bfloat16)
    vmem = pl.BlockSpec(memory_space=pltpu.VMEM)
    hbm = pl.BlockSpec(memory_space=pltpu.HBM)
    dma = pltpu.SemaphoreType.DMA
    regular = pltpu.SemaphoreType.REGULAR
    f32 = jnp.float32
    return pl.pallas_call(
        functools.partial(body, rows),
        out_shape=(whole, pltpu.VMEM((32, 128), jnp.bfloat16)),
        in_specs=[hbm] * 11,
        out_specs=(vmem,) * 2,
        scratch_shapes=[
            pltpu.VMEM((3, rows, width), jnp.bfloat16),
            pltpu.VMEM((3, rank, rows), jnp.bfloat16),
            pltpu.VMEM((3, rank, width), jnp.bfloat16),
            pltpu.VMEM((1, 16), f32),
            pltpu.VMEM((1, 16), f32),
            pltpu.VMEM((8, 4, 128), jnp.bfloat16),
            pltpu.VMEM((2, 8, 128), f32),
            pltpu.VMEM((4, 8, 128), f32),
            pltpu.VMEM((4, 8, 128), f32),
            pltpu.VMEM((32, 128), f32),
            dma((4, 3)),
            dma((flat(4, 0),)), dma((flat(4, 0),)), dma((flat_sib(NZ, 0),)),
            dma((1 + len(PIECES[3]),)), dma((1 + len(PIECES[3]),)), dma((1,)),
            dma((7,)), dma((7,)), dma, dma, dma((3,)), dma((3,)), dma((3,)), dma((3,)),
            regular, regular, regular, regular, regular, regular,
        ],
        compiler_params=pltpu.CompilerParams(collective_id=0, has_side_effects=True, vmem_limit_bytes=30 * 2**20),
        name="merge_and_gather",
    )(*[pltpu.with_memory_space_constraint(v, pltpu.HBM) for v in (*w, *a, *b, *norms)])


def write_out(blocks, row, gate, up, down, norm, sems):
    rows, width = gate.shape[0], blocks.shape[2]
    norm_copy = pltpu.make_async_copy(row, norm, sems.at[1])
    norm_copy.start()
    for f in range(blocks.shape[0]):
        for m, out in enumerate((gate, up, down)):
            pltpu.make_async_copy(
                blocks.at[f, pl.ds(m * rows, rows), :], out.at[:, pl.ds(f * width, width)], sems.at[0]).start()
    norm_copy.wait()
    pltpu.make_async_copy(blocks, blocks, sems.at[0]).wait()


def written(blocks, row):
    count, rows, width = blocks.shape
    whole = jax.ShapeDtypeStruct((rows // 3, count * width), blocks.dtype)
    return pl.pallas_call(
        write_out,
        out_shape=(whole, whole, whole, jax.ShapeDtypeStruct(row.shape, row.dtype)),
        in_specs=[pl.BlockSpec(memory_space=pltpu.VMEM)] * 2,
        out_specs=(pl.BlockSpec(memory_space=pltpu.HBM),) * 4,
        scratch_shapes=[pltpu.SemaphoreType.DMA((2,))],
        compiler_params=pltpu.CompilerParams(vmem_limit_bytes=2**20),
        name="write_out",
    )(blocks, row)


def local(w_gate, low_gate, high_gate, w_up, low_up, high_up, w_down, low_down, high_down, norm_train, norm_step):
    blocks, row = gathered(
        w_gate.T, w_up.T, w_down, high_gate, high_up, low_down.T, low_gate.T, low_up.T, high_down,
        norm_train.reshape(1, 16), norm_step.reshape(1, 16))
    gate, up, down, norm = written(blocks, row)
    return gate.T, up.T, down, norm.reshape(-1)


def solution(mesh):
    finer = Mesh(mesh.devices.reshape(8, 2, 4, 4), AXES)
    in_specs = (
        P(FSDP, TP), P(FSDP, None), P(None, TP),
        P(FSDP, TP), P(FSDP, None), P(None, TP),
        P(TP, FSDP), P(TP, None), P(None, FSDP),
        P(FSDP + TP), P(FSDP + TP),
    )
    out_specs = (P(None, TP), P(None, TP), P(TP, None), P())
    return jax.shard_map(local, mesh=finer, in_specs=in_specs, out_specs=out_specs, check_vma=False)
```
